32 devices in a mesh: grp: 2 (over x), sp: 16 (over z, y, core).
Axes of the slice: x: 2, y: 2, z: 4, core: 2. Of those that a mesh axis runs over, the one named last changes fastest.
Arguments:
- video_query: bfloat16 [4, 16, 2048, 128], P('grp', None, 'sp'), parts along dimension 0, may hold values from -6 to 6
- video_key: bfloat16 [4, 16, 2048, 128], P('grp', None, 'sp'), parts along dimension 0, may hold values from -6 to 6
- video_value: bfloat16 [4, 16, 2048, 128], P('grp', None, 'sp'), parts along dimension 0, may hold values from -6 to 6
- text_query: bfloat16 [4, 16, 256, 128], P('grp', None, 'sp'), parts along dimension 0, may hold values from -6 to 6
- text_key: bfloat16 [4, 16, 256, 128], P('grp', None, 'sp'), parts along dimension 0, may hold values from -6 to 6
- text_value: bfloat16 [4, 16, 256, 128], P('grp', None, 'sp'), parts along dimension 0, may hold values from -6 to 6
- positions: int32 [6, 2048], P('grp', 'sp'), parts along dimension 0, may hold values from 0 to 63
- text_lengths: int32 [4], P('grp'), parts along dimension 0, may hold values from 1 to 256
- query_gain: float32 [128], replicated, may hold values from 1 to 2.2
- key_gain: float32 [128], replicated, may hold values from 1 to 2.2
- out_weight: bfloat16 [2048, 3072], replicated, may hold values from -0.125 to 0.125
- branch_gates: float32 [4, 3072], P('grp'), parts along dimension 0, may hold values from -3 to 3
- video_stream: bfloat16 [4, 2048, 3072], P('grp', 'sp'), parts along dimension 0, may hold values from -6 to 6
- text_stream: bfloat16 [4, 256, 3072], P('grp', 'sp'), parts along dimension 0, may hold values from -6 to 6
Outputs:
- guided: bfloat16 [2048, 6144], P('sp', 'grp'), parts along dimension 1
- video_next: bfloat16 [4, 2048, 3072], P('grp', 'sp'), parts along dimension 0
- text_next: bfloat16 [4, 256, 3072], P('grp', 'sp'), parts along dimension 0
The draws below stay inside these ranges and needn't reach their ends.
There are 2 independent parts, one for each index of `grp`. The reference program is written for one: setup_inputs(seed, part) draws one part's arguments, and reference() takes and returns one part's arrays. A program takes and returns all parts, laid end to end along the dimension named above; an argument that names none is the same for every part. Nothing has to cross between parts.
Inputs may be any that keep to these rules, and one draw needn't show every extreme that they name: Entry 0 counts the conditional prompt's text tokens, entry 1 the unconditional one's; text tokens at index text_lengths[b] or later are padding.
All inputs are finite; a program needn't handle non-finite values.
Results may differ from the reference program's by a relative error of at most 0.0054.
Values may be sent and summed in bfloat16 or wider, within the bound.
A program may use at most 128 MiB of HBM per device.

```python
import math
import jax
import jax.numpy as jnp
from jax import lax

WIDTH = 3072
HEADS = 16
HEAD = 128
TEXT = 256
VIDEO = 2048


def plant(values, rng, least, high):
    dims = values.shape
    spot = [jax.random.randint(jax.random.fold_in(rng, axis), (), 0, dims[axis]) for axis in range(len(dims))]
    values = values.at[tuple(spot)].set(least)
    longest = dims.index(max(dims))
    spot[longest] = (spot[longest] + 1) % dims[longest]
    return values.at[tuple(spot)].set(high)


def shard_levels(key, extent, shards, smallest, top_value):
    def one(axis_at, shards_of):
        heights = jax.random.uniform(jax.random.fold_in(jax.random.fold_in(key, 6), axis_at), (shards_of,), jnp.float32, smallest / len(shards), top_value / len(shards))
        return jnp.repeat(jnp.exp(heights), extent[axis_at] // shards_of).reshape((-1,) + (1,) * (len(extent) - axis_at - 1))

    gain = one(*shards[0])
    for cut in shards[1:]:
        gain = gain * one(*cut)
    return gain


def gaussian(key, dims, width, limit, shards=(), kind=jnp.bfloat16):
    entries = width * jax.random.normal(key, dims, jnp.float32)
    if shards:
        entries = entries * shard_levels(key, dims, shards, -0.22, 0.18)
    return jnp.clip(entries, -limit, limit).astype(kind)


def setup_inputs(seed: int = 0, part: int = 0) -> dict:
    splits = jax.random.split(jax.random.key(seed), 15)
    own_keys = jax.random.split(jax.random.fold_in(splits[14], part), 15)
    video_query = gaussian(own_keys[0], (2, HEADS, VIDEO, HEAD), 1.0, 6.0, ((2, 16),))
    video_key = gaussian(own_keys[1], (2, HEADS, VIDEO, HEAD), 1.0, 6.0, ((2, 16),))
    video_value = gaussian(own_keys[2], (2, HEADS, VIDEO, HEAD), 1.0, 6.0, ((2, 16),))
    text_query = gaussian(own_keys[3], (2, HEADS, TEXT, HEAD), 1.0, 6.0, ((2, 16),))
    text_key = gaussian(own_keys[4], (2, HEADS, TEXT, HEAD), 1.0, 6.0, ((2, 16),))
    text_value = gaussian(own_keys[5], (2, HEADS, TEXT, HEAD), 1.0, 6.0, ((2, 16),))
    positions = plant(jax.random.randint(own_keys[6], (3, VIDEO), 0, 64), jax.random.fold_in(own_keys[6], 1), 0, 63).astype(jnp.int32)
    text_lengths = jax.random.randint(own_keys[7], (2,), 1, TEXT + 1).astype(jnp.int32)
    query_gain = jnp.clip(jnp.exp(jax.random.uniform(splits[8], (HEAD,), jnp.float32, math.log(1.0), math.log(2.2))), 1.0, 2.2)
    key_gain = jnp.clip(jnp.exp(jax.random.uniform(splits[9], (HEAD,), jnp.float32, math.log(1.0), math.log(2.2))), 1.0, 2.2)
    out_weight = gaussian(splits[10], (HEADS * HEAD, WIDTH), (HEADS * HEAD) ** -0.5, 0.125)
    branch_gates = gaussian(own_keys[11], (2, WIDTH), 1.0, 3.0, (), jnp.float32)
    video_stream = gaussian(own_keys[12], (2, VIDEO, WIDTH), 1.0, 6.0, ((1, 16),))
    text_stream = gaussian(own_keys[13], (2, TEXT, WIDTH), 1.0, 6.0, ((1, 16),))
    return dict(video_query=video_query, video_key=video_key, video_value=video_value, text_query=text_query, text_key=text_key, text_value=text_value, positions=positions, text_lengths=text_lengths, query_gain=query_gain, key_gain=key_gain, out_weight=out_weight, branch_gates=branch_gates, video_stream=video_stream, text_stream=text_stream)


norm_eps = 1e-06
rope_theta = 256.0
guidance_scale = 5.0

def rope_tables(positions, head_dim):
    frame_width = head_dim // 8
    side_width = 7 * head_dim // 16
    starts = (0, frame_width, frame_width + side_width)
    extents = (frame_width, side_width, side_width)
    channel = jnp.arange(head_dim, dtype=jnp.int32)
    angles = jnp.zeros((positions.shape[1], head_dim), jnp.float32)
    for axis_slot in range(3):
        inside = (channel >= starts[axis_slot]) & (channel < starts[axis_slot] + extents[axis_slot])
        within = ((channel - starts[axis_slot]) // 2).astype(jnp.float32)
        frequency = jnp.where(inside, jnp.exp(-2.0 * within / extents[axis_slot] * math.log(rope_theta)), 0.0).astype(jnp.float32)
        angles = angles + positions[axis_slot].astype(jnp.float32)[:, None] * frequency[None, :]
    return (jnp.cos(angles), jnp.sin(angles))

def rms_scale(values, gain_vector):
    widened = values.astype(jnp.float32)
    return widened * lax.rsqrt(lax.optimization_barrier(jnp.mean(widened * widened, axis=-1, keepdims=True)) + norm_eps) * gain_vector

def rotate_pairs(values, cosine_table, sine_table):
    is_even = jnp.arange(values.shape[-1], dtype=jnp.int32) % 2 == 0
    partner = jnp.where(is_even, -jnp.roll(values, -1, axis=-1), jnp.roll(values, 1, axis=-1))
    return values * cosine_table + partner * sine_table

def prepare_rotated(values, gain_vector, cosine_table, sine_table):
    return rotate_pairs(rms_scale(values, gain_vector), cosine_table, sine_table).astype(jnp.bfloat16)

def prepare_plain(values, gain_vector):
    return rms_scale(values, gain_vector).astype(jnp.bfloat16)

def block_rows(overall):
    chosen = min(overall, 1024)
    while overall % chosen:
        chosen -= 1
    return chosen

def attend_one(query_rows, key_rows, value_rows, key_mask, score_scale):
    overall, head_dim = query_rows.shape
    chosen = block_rows(overall)
    wide_keys = key_rows.astype(jnp.float32)
    wide_values = value_rows.astype(jnp.float32)
    grouped = query_rows.reshape(overall // chosen, chosen, head_dim)

    def one_block(rows_block):
        scores = jnp.einsum('qd,kd->qk', rows_block.astype(jnp.float32), wide_keys) * score_scale
        weights = jnp.exp(scores) * key_mask[None, :]
        denominator = lax.optimization_barrier(jnp.sum(weights, axis=-1, keepdims=True))
        rounded = lax.optimization_barrier(weights.astype(jnp.bfloat16)).astype(jnp.float32)
        summed = jnp.einsum('qk,kd->qd', rounded, wide_values)
        return (summed / denominator).astype(jnp.bfloat16)
    return lax.map(one_block, grouped).reshape(overall, head_dim)

def advance(attended, stream, weight_heads, gate_rows):
    projected = jnp.einsum('bhrd,hde->bre', attended.astype(jnp.float32), weight_heads.astype(jnp.float32))
    return stream.astype(jnp.float32) + gate_rows[:, None, :] * projected

def reference(video_query, video_key, video_value, text_query, text_key, text_value, positions, text_lengths, query_gain, key_gain, out_weight, branch_gates, video_stream, text_stream):
    head_count = video_query.shape[1]
    head_dim = video_query.shape[3]
    video_rows = video_query.shape[2]
    text_rows = text_query.shape[2]
    item_count = 2 * head_count
    score_scale = head_dim ** (-0.5)
    cosine_table, sine_table = rope_tables(positions, head_dim)
    video_queries = prepare_rotated(video_query, query_gain, cosine_table, sine_table).reshape(item_count, video_rows, head_dim)
    video_keys = prepare_rotated(video_key, key_gain, cosine_table, sine_table).reshape(item_count, video_rows, head_dim)
    text_queries = prepare_plain(text_query, query_gain).reshape(item_count, text_rows, head_dim)
    text_keys = prepare_plain(text_key, key_gain).reshape(item_count, text_rows, head_dim)
    queries = jnp.concatenate([video_queries, text_queries], axis=1)
    key_rows = jnp.concatenate([video_keys, text_keys], axis=1)
    value_rows = jnp.concatenate([video_value.reshape(item_count, video_rows, head_dim), text_value.reshape(item_count, text_rows, head_dim)], axis=1)
    branch_of = jnp.arange(item_count, dtype=jnp.int32) // head_count
    limits = jnp.where(branch_of == 0, text_lengths[0], text_lengths[1])
    text_mask = (jnp.arange(text_rows, dtype=jnp.int32)[None, :] < limits[:, None]).astype(jnp.float32)
    masks = jnp.concatenate([jnp.ones((item_count, video_rows), jnp.float32), text_mask], axis=1)

    def attend_packed(packed):
        return attend_one(packed[0], packed[1], packed[2], packed[3], score_scale)
    attended = lax.map(attend_packed, (queries, key_rows, value_rows, masks))
    video_out = attended[:, :video_rows].reshape(2, head_count, video_rows, head_dim)
    text_out = attended[:, video_rows:].reshape(2, head_count, text_rows, head_dim)
    weight_heads = out_weight.reshape(head_count, head_dim, out_weight.shape[1])
    video_streams = advance(video_out, video_stream, weight_heads, branch_gates)
    text_streams = advance(text_out, text_stream, weight_heads, branch_gates)
    guided = (video_streams[1] + guidance_scale * (video_streams[0] - video_streams[1])).astype(jnp.bfloat16)
    return (guided, video_streams.astype(jnp.bfloat16), text_streams.astype(jnp.bfloat16))
```

```python
import functools
import math

import jax
import jax.numpy as jnp
from jax import lax
from jax.experimental import pallas as pl
from jax.experimental.pallas import tpu as pltpu
from jax.sharding import PartitionSpec as P

norm_eps = 1e-06
rope_theta = 256.0
guidance_scale = 5.0

MESH = pl.DeviceIdType.MESH
F32 = jnp.float32
BF16 = jnp.bfloat16
V, K, Q, O = 0, 1, 2, 3


def swapped(rows):
    even = lax.broadcasted_iota(jnp.int32, rows.shape, 1) % 2 == 0
    last = rows.shape[1] - 1
    return jnp.where(even, pltpu.roll(rows, last, 1), pltpu.roll(rows, 1, 1))


def rope_tables(positions, head_dim):
    frame_width = head_dim // 8
    side_width = 7 * head_dim // 16
    starts = (0, frame_width, frame_width + side_width)
    extents = (frame_width, side_width, side_width)
    tokens = positions.shape[1]
    channel = lax.broadcasted_iota(jnp.int32, (head_dim, tokens), 0)
    angles = jnp.zeros((head_dim, tokens), F32)
    for slot in range(3):
        inside = (channel >= starts[slot]) & (channel < starts[slot] + extents[slot])
        within = ((channel - starts[slot]) // 2).astype(F32)
        frequency = jnp.where(
            inside, jnp.exp(-2.0 * within / extents[slot] * math.log(rope_theta)), 0.0
        )
        angles = angles + positions[slot : slot + 1, :].astype(F32) * frequency
    return jnp.cos(angles).T, jnp.sin(angles).T


def kernel(
    n,
    heads,
    chunk,
    group,
    vq_ref,
    vk_ref,
    vv_ref,
    tq_ref,
    tk_ref,
    tv_ref,
    pos_ref,
    len_ref,
    qg_ref,
    kg_ref,
    weight_hbm,
    gate_ref,
    vstream_hbm,
    tstream_hbm,
    guided_ref,
    vnext_ref,
    tnext_ref,
    comb,
    got,
    osend,
    ohome,
    vext,
    tables,
    weight,
    vstream,
    tstream,
    acc,
    send_sem,
    recv_sem,
    local_sem,
):
    me = lax.axis_index("sp")
    items, rows_v, head_dim = vq_ref.shape
    rows_t = tq_ref.shape[1]
    rows = comb.shape[2]
    waves = items // n
    width = weight.shape[1]

    barrier = pltpu.get_barrier_semaphore()

    @pl.loop(1, n)
    def _(i):
        pl.semaphore_signal(
            barrier, inc=1, device_id={"sp": lax.rem(me + i, n)}, device_id_type=MESH
        )

    loads = (
        pltpu.make_async_copy(weight_hbm, weight, local_sem.at[0]),
        pltpu.make_async_copy(vstream_hbm, vstream, local_sem.at[1]),
        pltpu.make_async_copy(tstream_hbm, tstream, local_sem.at[2]),
    )
    for load in loads:
        load.start()

    def copy_in(kind, wave, owner, target):
        return pltpu.make_async_remote_copy(
            src_ref=comb.at[kind, wave * n + target],
            dst_ref=got.at[kind, wave, owner],
            send_sem=send_sem.at[kind, wave, target],
            recv_sem=recv_sem.at[kind, wave, owner],
            device_id={"sp": target},
            device_id_type=MESH,
        )

    def copy_back(wave, owner, target):
        return pltpu.make_async_remote_copy(
            src_ref=osend.at[wave, target],
            dst_ref=ohome.at[wave * n + owner],
            send_sem=send_sem.at[O, wave, target],
            recv_sem=recv_sem.at[O, wave, owner],
            device_id={"sp": target},
            device_id_type=MESH,
        )

    def deal(kind, wave, make):
        @pl.loop(0, n)
        def _(i):
            target = lax.rem(me + i, n)
            video, text = make(wave * n + target)

            def put(ref):
                ref[pl.ds(0, rows_v), :] = video
                ref[pl.ds(rows_v, rows_t), :] = text
                if rows > rows_v + rows_t:
                    spare = rows - rows_v - rows_t
                    ref[pl.ds(rows_v + rows_t, spare), :] = jnp.zeros((spare, head_dim), BF16)

            @pl.when(target == me)
            def _():
                put(got.at[kind, wave, me])

            @pl.when(target != me)
            def _():
                put(comb.at[kind, wave * n + target])
                copy_in(kind, wave, me, target).start()

    def make_value(item):
        return vv_ref[item], tv_ref[item]

    def inverse_rms(wide):
        return lax.rsqrt(jnp.mean(wide * wide, axis=-1, keepdims=True) + norm_eps)

    source = lax.broadcasted_iota(jnp.int32, (head_dim, head_dim), 0)
    dest = lax.broadcasted_iota(jnp.int32, (head_dim, head_dim), 1)
    partner_of = jnp.where(
        (dest % 2 == 0) & (source == dest + 1),
        -1.0,
        jnp.where((dest % 2 == 1) & (source == dest - 1), 1.0, 0.0),
    ).astype(BF16)

    def make_normed(video_ref, text_ref, slot, gain):
        def make(item):
            raw = video_ref[item]
            wide = raw.astype(F32)
            partner = jnp.dot(raw, partner_of, preferred_element_type=F32)
            video = inverse_rms(wide) * (
                wide * tables[slot, 0] + partner * tables[slot, 1]
            )
            plain = text_ref[item].astype(F32)
            text = plain * inverse_rms(plain) * gain
            return video.astype(BF16), text.astype(BF16)

        return make

    pl.semaphore_wait(barrier, n - 1)
    deal(V, 0, make_value)

    query_gain = qg_ref[...] * (head_dim ** (-0.5) * math.log2(math.e))
    key_gain = kg_ref[...]
    cosine, sine = rope_tables(pos_ref[...], head_dim)
    for slot, gain in ((0, key_gain), (1, query_gain)):
        tall = jnp.broadcast_to(gain, (8, head_dim))
        tables[slot, 0] = cosine * gain
        tables[slot, 1] = sine * swapped(tall)[0:1, :]

    make_key = make_normed(vk_ref, tk_ref, 0, key_gain)
    make_query = make_normed(vq_ref, tq_ref, 1, query_gain)
    for wave in range(waves):
        if wave > 0:
            deal(V, wave, make_value)
        deal(K, wave, make_key)
        deal(Q, wave, make_query)

    acc[...] = jnp.zeros_like(acc)

    row = lax.broadcasted_iota(jnp.int32, (rows, 1), 0)
    for wave in range(waves):
        limit = len_ref[(wave * n + me) // heads]

        @pl.loop(0, n)
        def _(owner):
            @pl.when(owner != me)
            def _():
                copy_in(V, wave, owner, me).wait_recv()
                copy_in(K, wave, owner, me).wait_recv()

            text_index = owner * rows_t + row - rows_v
            live = (row < rows_v) | ((row < rows_v + rows_t) & (text_index < limit))
            counted = jnp.broadcast_to(jnp.where(live, 1.0, 0.0), (rows, head_dim)).astype(BF16)
            vext[owner, :, pl.ds(0, head_dim)] = got[V, wave, owner] * counted
            vext[owner, :, pl.ds(head_dim, head_dim)] = counted

        @pl.loop(0, n // chunk)
        def _(step):
            first = lax.rem(me // chunk + step, n // chunk) * chunk
            for j in range(chunk):

                @pl.when(first + j != me)
                def _():
                    copy_in(Q, wave, first + j, me).wait_recv()

            queries = got[Q, wave, pl.ds(first, chunk)].reshape(chunk * rows, head_dim)
            keys = got[K, wave].reshape(n * rows, head_dim)
            scores = lax.dot_general(
                queries, keys, (((1,), (1,)), ((), ())), preferred_element_type=F32
            )
            weights = jnp.exp2(scores).astype(BF16)
            summed = jnp.dot(
                weights, vext[...].reshape(n * rows, 2 * head_dim), preferred_element_type=F32
            )
            attended = (summed[:, :head_dim] / summed[:, head_dim:]).astype(BF16)
            for j in range(chunk):
                part = attended[j * rows : (j + 1) * rows]

                @pl.when(first + j == me)
                def _():
                    ohome[wave * n + me] = part

                @pl.when(first + j != me)
                def _():
                    osend[wave, first + j] = part
                    copy_back(wave, me, first + j).start()

    loads[0].wait()
    tile = math.gcd(width, 768)
    for wave in range(waves):

        @pl.loop(0, n // group)
        def _(step):
            first = lax.rem(me // group + n // group - step, n // group) * group
            for j in range(group):

                @pl.when(first + j != me)
                def _():
                    copy_back(wave, first + j, me).wait_recv()

            item = wave * n + first
            branch, head = item // heads, lax.rem(item, heads)
            rows_in = jnp.concatenate([ohome[item + j] for j in range(group)], axis=1)

            @pl.loop(0, width // tile)
            def _(t):
                columns = pl.ds(pl.multiple_of(t * tile, tile), tile)
                depth = pl.ds(pl.multiple_of(head * head_dim, head_dim), group * head_dim)
                acc[branch, :, columns] += jnp.dot(
                    rows_in, weight[depth, columns], preferred_element_type=F32
                )

    loads[1].wait()
    loads[2].wait()

    @pl.loop(0, width // tile)
    def _(t):
        columns = pl.ds(pl.multiple_of(t * tile, tile), tile)
        streams = []
        for branch in range(2):
            gate = gate_ref[pl.ds(branch, 1), columns]
            stream = vstream[branch, :, columns].astype(F32) + gate * acc[
                branch, pl.ds(0, rows_v), columns
            ]
            vnext_ref[branch, :, columns] = stream.astype(BF16)
            streams.append(stream)
            tnext_ref[branch, :, columns] = (
                tstream[branch, :, columns].astype(F32)
                + gate * acc[branch, pl.ds(rows_v, rows_t), columns]
            ).astype(BF16)
        guided_ref[:, columns] = (
            streams[1] + guidance_scale * (streams[0] - streams[1])
        ).astype(BF16)

    for wave in range(waves):

        @pl.loop(1, n)
        def _(i):
            target = lax.rem(me + i, n)
            for kind in (V, K, Q):
                copy_in(kind, wave, me, target).wait_send()
            copy_back(wave, me, target).wait_send()


def body(
    n,
    video_query,
    video_key,
    video_value,
    text_query,
    text_key,
    text_value,
    positions,
    text_lengths,
    query_gain,
    key_gain,
    out_weight,
    branch_gates,
    video_stream,
    text_stream,
):
    branches, heads, rows_v, head_dim = video_query.shape
    rows_t = text_query.shape[2]
    items = branches * heads
    waves = items // n
    rows = -(-(rows_v + rows_t) // 16) * 16
    width = out_weight.shape[1]
    chunk = 2 if n % 2 == 0 else 1
    group = math.gcd(math.gcd(n, heads), 4)

    def flat(tensor):
        return tensor.reshape((items,) + tensor.shape[2:])

    vmem = pl.BlockSpec(memory_space=pltpu.VMEM)
    smem = pl.BlockSpec(memory_space=pltpu.SMEM)
    anywhere = pl.BlockSpec(memory_space=pl.ANY)
    return pl.pallas_call(
        functools.partial(kernel, n, heads, chunk, group),
        out_shape=(
            jax.ShapeDtypeStruct((rows_v, width), BF16),
            jax.ShapeDtypeStruct((branches, rows_v, width), BF16),
            jax.ShapeDtypeStruct((branches, rows_t, width), BF16),
        ),
        in_specs=[vmem] * 7 + [smem, vmem, vmem, anywhere, vmem, anywhere, anywhere],
        out_specs=(vmem, vmem, vmem),
        scratch_shapes=[
            pltpu.VMEM((3, items, rows, head_dim), BF16),
            pltpu.VMEM((3, waves, n, rows, head_dim), BF16),
            pltpu.VMEM((waves, n, rows, head_dim), BF16),
            pltpu.VMEM((items, rows, head_dim), BF16),
            pltpu.VMEM((n, rows, 2 * head_dim), BF16),
            pltpu.VMEM((2, 2, rows_v, head_dim), F32),
            pltpu.VMEM(out_weight.shape, BF16),
            pltpu.VMEM(video_stream.shape, BF16),
            pltpu.VMEM(text_stream.shape, BF16),
            pltpu.VMEM((branches, rows, width), F32),
            pltpu.SemaphoreType.DMA((4, waves, n)),
            pltpu.SemaphoreType.DMA((4, waves, n)),
            pltpu.SemaphoreType.DMA((3,)),
        ],
        compiler_params=pltpu.CompilerParams(
            collective_id=0, has_side_effects=True, vmem_limit_bytes=63 * 1024 * 1024
        ),
    )(
        flat(video_query),
        flat(video_key),
        flat(video_value),
        flat(text_query),
        flat(text_key),
        flat(text_value),
        positions,
        text_lengths,
        query_gain.reshape(1, head_dim),
        key_gain.reshape(1, head_dim),
        out_weight,
        branch_gates,
        video_stream,
        text_stream,
    )


def solution(mesh):
    return jax.shard_map(
        functools.partial(body, mesh.shape["sp"]),
        mesh=mesh,
        in_specs=(
            P("grp", None, "sp", None),
            P("grp", None, "sp", None),
            P("grp", None, "sp", None),
            P("grp", None, "sp", None),
            P("grp", None, "sp", None),
            P("grp", None, "sp", None),
            P("grp", "sp"),
            P("grp"),
            P(),
            P(),
            P(),
            P("grp", None),
            P("grp", "sp", None),
            P("grp", "sp", None),
        ),
        out_specs=(P("sp", "grp"), P("grp", "sp", None), P("grp", "sp", None)),
        check_vma=False,
    )
```

```python
import functools
import math

import jax
import jax.numpy as jnp
from jax import lax
from jax.experimental import pallas as pl
from jax.experimental.pallas import tpu as pltpu
from jax.sharding import PartitionSpec as P

norm_eps = 1e-06
rope_theta = 256.0
guidance_scale = 5.0

MESH = pl.DeviceIdType.MESH
F32 = jnp.float32
BF16 = jnp.bfloat16
V, K, Q, O = 0, 1, 2, 3


def swapped(rows):
    even = lax.broadcasted_iota(jnp.int32, rows.shape, 1) % 2 == 0
    last = rows.shape[1] - 1
    return jnp.where(even, pltpu.roll(rows, last, 1), pltpu.roll(rows, 1, 1))


def rope_tables(positions, head_dim):
    frame_width = head_dim // 8
    side_width = 7 * head_dim // 16
    starts = (0, frame_width, frame_width + side_width)
    extents = (frame_width, side_width, side_width)
    tokens = positions.shape[1]
    channel = lax.broadcasted_iota(jnp.int32, (head_dim, tokens), 0)
    angles = jnp.zeros((head_dim, tokens), F32)
    for slot in range(3):
        inside = (channel >= starts[slot]) & (channel < starts[slot] + extents[slot])
        within = ((channel - starts[slot]) // 2).astype(F32)
        frequency = jnp.where(
            inside, jnp.exp(-2.0 * within / extents[slot] * math.log(rope_theta)), 0.0
        )
        angles = angles + positions[slot : slot + 1, :].astype(F32) * frequency
    return jnp.cos(angles).T, jnp.sin(angles).T


def kernel(
    n,
    heads,
    chunk,
    group,
    vv_hbm,
    tv_hbm,
    vk_hbm,
    tk_hbm,
    vq_hbm,
    tq_hbm,
    pos_ref,
    len_ref,
    qg_ref,
    kg_ref,
    weight_hbm,
    proj_hbm,
    vv_ref,
    tv_ref,
    vk_ref,
    tk_ref,
    vq_ref,
    tq_ref,
    comb,
    got,
    osend,
    ohome,
    vext,
    tables,
    weight,
    acc,
    send_sem,
    recv_sem,
    local_sem,
    out_sem,
):
    me = lax.axis_index("sp")
    items, rows_v, head_dim = vq_ref.shape
    rows_t = tq_ref.shape[1]
    rows = comb.shape[2]
    waves = items // n
    width = weight.shape[1]

    barrier = pltpu.get_barrier_semaphore()

    @pl.loop(1, n)
    def _(i):
        pl.semaphore_signal(
            barrier, inc=1, device_id={"sp": lax.rem(me + i, n)}, device_id_type=MESH
        )

    sources = (vv_hbm, tv_hbm, vk_hbm, tk_hbm, vq_hbm, tq_hbm, weight_hbm)
    places = (vv_ref, tv_ref, vk_ref, tk_ref, vq_ref, tq_ref, weight)
    loads = [
        pltpu.make_async_copy(there, here, local_sem.at[i])
        for i, (there, here) in enumerate(zip(sources, places))
    ]
    for load in loads[:6]:
        load.start()

    half = n // 2
    side = me // half

    def far_first(i, size):
        blocks = half // size
        other = lax.rem(side + 1 + i // blocks, 2)
        return (other * blocks + lax.rem(me // size + i, blocks)) * size

    def copy_in(kind, wave, owner, target):
        return pltpu.make_async_remote_copy(
            src_ref=comb.at[kind, wave * n + target],
            dst_ref=got.at[kind, wave, owner],
            send_sem=send_sem.at[kind, wave, target],
            recv_sem=recv_sem.at[kind, wave, owner],
            device_id={"sp": target},
            device_id_type=MESH,
        )

    def copy_back(wave, owner, target):
        return pltpu.make_async_remote_copy(
            src_ref=osend.at[wave, target],
            dst_ref=ohome.at[wave * n + owner],
            send_sem=send_sem.at[O, wave, target],
            recv_sem=recv_sem.at[O, wave, owner],
            device_id={"sp": target},
            device_id_type=MESH,
        )

    def deal(kind, wave, make):
        @pl.loop(0, n)
        def _(i):
            target = far_first(i, 1)
            video, text = make(wave * n + target)

            def put(ref):
                ref[pl.ds(0, rows_v), :] = video
                ref[pl.ds(rows_v, rows_t), :] = text
                if rows > rows_v + rows_t:
                    spare = rows - rows_v - rows_t
                    ref[pl.ds(rows_v + rows_t, spare), :] = jnp.zeros((spare, head_dim), BF16)

            @pl.when(target == me)
            def _():
                put(got.at[kind, wave, me])

            @pl.when(target != me)
            def _():
                put(comb.at[kind, wave * n + target])
                copy_in(kind, wave, me, target).start()

    def make_value(item):
        return vv_ref[item], tv_ref[item]

    def inverse_rms(wide):
        return lax.rsqrt(jnp.mean(wide * wide, axis=-1, keepdims=True) + norm_eps)

    source = lax.broadcasted_iota(jnp.int32, (head_dim, head_dim), 0)
    dest = lax.broadcasted_iota(jnp.int32, (head_dim, head_dim), 1)
    partner_of = jnp.where(
        (dest % 2 == 0) & (source == dest + 1),
        -1.0,
        jnp.where((dest % 2 == 1) & (source == dest - 1), 1.0, 0.0),
    ).astype(BF16)

    def make_normed(video_ref, text_ref, slot, gain):
        def make(item):
            raw = video_ref[item]
            wide = raw.astype(F32)
            partner = jnp.dot(raw, partner_of, preferred_element_type=F32)
            video = inverse_rms(wide) * (
                wide * tables[slot, 0] + partner * tables[slot, 1]
            )
            plain = text_ref[item].astype(F32)
            text = plain * inverse_rms(plain) * gain
            return video.astype(BF16), text.astype(BF16)

        return make

    loads[0].wait()
    loads[1].wait()
    pl.semaphore_wait(barrier, n - 1)
    deal(V, 0, make_value)

    query_gain = qg_ref[...]
    key_gain = kg_ref[...]
    cosine, sine = rope_tables(pos_ref[...], head_dim)
    for slot, gain in ((0, key_gain), (1, query_gain)):
        tall = jnp.broadcast_to(gain, (8, head_dim))
        tables[slot, 0] = cosine * gain
        tables[slot, 1] = sine * swapped(tall)[0:1, :]

    make_key = make_normed(vk_ref, tk_ref, 0, key_gain)
    make_query = make_normed(vq_ref, tq_ref, 1, query_gain)
    for load in loads[2:6]:
        load.wait()
    loads[6].start()
    for wave in range(waves):
        if wave > 0:
            deal(V, wave, make_value)
        deal(K, wave, make_key)
        deal(Q, wave, make_query)

    acc[...] = jnp.zeros_like(acc)

    score_scale = head_dim ** (-0.5) * math.log2(math.e)
    row = lax.broadcasted_iota(jnp.int32, (rows, 1), 0)
    for wave in range(waves):
        limit = len_ref[(wave * n + me) // heads]

        @pl.loop(0, n)
        def _(owner):
            @pl.when(owner != me)
            def _():
                copy_in(V, wave, owner, me).wait_recv()
                copy_in(K, wave, owner, me).wait_recv()

            text_index = owner * rows_t + row - rows_v
            live = (row < rows_v) | ((row < rows_v + rows_t) & (text_index < limit))
            counted = jnp.broadcast_to(jnp.where(live, 1.0, 0.0), (rows, head_dim)).astype(BF16)
            vext[owner, :, pl.ds(0, head_dim)] = got[V, wave, owner] * counted
            vext[owner, :, pl.ds(head_dim, head_dim)] = counted

        @pl.loop(0, n // chunk)
        def _(step):
            first = far_first(step, chunk)
            for j in range(chunk):

                @pl.when(first + j != me)
                def _():
                    copy_in(Q, wave, first + j, me).wait_recv()

            queries = got[Q, wave, pl.ds(first, chunk)].reshape(chunk * rows, head_dim)
            keys = got[K, wave].reshape(n * rows, head_dim)
            scores = lax.dot_general(
                queries, keys, (((1,), (1,)), ((), ())), preferred_element_type=F32
            )
            weights = jnp.exp2(scores * score_scale).astype(BF16)
            summed = jnp.dot(
                weights, vext[...].reshape(n * rows, 2 * head_dim), preferred_element_type=F32
            )
            attended = (summed[:, :head_dim] / summed[:, head_dim:]).astype(BF16)
            for j in range(chunk):
                part = attended[j * rows : (j + 1) * rows]

                @pl.when(first + j == me)
                def _():
                    ohome[wave * n + me] = part

                @pl.when(first + j != me)
                def _():
                    osend[wave, first + j] = part
                    copy_back(wave, me, first + j).start()

    loads[6].wait()
    tile = math.gcd(width, 768)
    count = heads // group

    def write(branch, t):
        columns = pl.ds(pl.multiple_of(t * tile, tile), tile)
        return pltpu.make_async_copy(
            acc.at[branch, :, columns], proj_hbm.at[branch, :, columns], out_sem.at[branch, t]
        )

    for branch in range(items // heads):
        wave, start = divmod(branch * heads, n)

        @pl.loop(0, count)
        def _(step):
            if count * group == n:
                first = far_first(step, group)
            else:
                first = start + step * group
            for j in range(group):

                @pl.when(first + j != me)
                def _():
                    copy_back(wave, first + j, me).wait_recv()

            item = wave * n + first
            head = item - branch * heads
            rows_in = jnp.concatenate([ohome[item + j] for j in range(group)], axis=1)

            @pl.loop(0, width // tile)
            def _(t):
                columns = pl.ds(pl.multiple_of(t * tile, tile), tile)
                depth = pl.ds(pl.multiple_of(head * head_dim, head_dim), group * head_dim)
                acc[branch, :, columns] += jnp.dot(
                    rows_in, weight[depth, columns], preferred_element_type=F32
                )

                @pl.when(step == count - 1)
                def _():
                    write(branch, t).start()

    for wave in range(waves):

        @pl.loop(1, n)
        def _(i):
            target = lax.rem(me + i, n)
            for kind in (V, K, Q):
                copy_in(kind, wave, me, target).wait_send()
            copy_back(wave, me, target).wait_send()

    for branch in range(items // heads):
        for t in range(width // tile):
            write(branch, t).wait()


def finish(proj_ref, gate_ref, vstream_ref, tstream_ref, guided_ref, vnext_ref, tnext_ref):
    rows_v, rows_t = vstream_ref.shape[1], tstream_ref.shape[1]
    streams = []
    for branch in range(2):
        gate = gate_ref[branch : branch + 1, :]
        stream = vstream_ref[branch].astype(F32) + gate * proj_ref[branch, :rows_v]
        vnext_ref[branch] = stream.astype(BF16)
        streams.append(stream)
        tnext_ref[branch] = (
            tstream_ref[branch].astype(F32) + gate * proj_ref[branch, rows_v : rows_v + rows_t]
        ).astype(BF16)
    guided_ref[...] = (streams[1] + guidance_scale * (streams[0] - streams[1])).astype(BF16)


def body(
    n,
    video_query,
    video_key,
    video_value,
    text_query,
    text_key,
    text_value,
    positions,
    text_lengths,
    query_gain,
    key_gain,
    out_weight,
    branch_gates,
    video_stream,
    text_stream,
):
    branches, heads, rows_v, head_dim = video_query.shape
    rows_t = text_query.shape[2]
    items = branches * heads
    waves = items // n
    rows = -(-(rows_v + rows_t) // 16) * 16
    width = out_weight.shape[1]
    chunk = 2 if n % 2 == 0 else 1
    group = math.gcd(math.gcd(n, heads), 4)

    def flat(tensor):
        return tensor.reshape((items,) + tensor.shape[2:])

    vmem = pl.BlockSpec(memory_space=pltpu.VMEM)
    smem = pl.BlockSpec(memory_space=pltpu.SMEM)
    anywhere = pl.BlockSpec(memory_space=pl.ANY)
    tile = math.gcd(width, 768)
    projected = pl.pallas_call(
        functools.partial(kernel, n, heads, chunk, group),
        out_shape=jax.ShapeDtypeStruct((branches, rows, width), F32),
        in_specs=[anywhere] * 6 + [vmem, smem, vmem, vmem, anywhere],
        out_specs=anywhere,
        scratch_shapes=[
            pltpu.VMEM((items, rows_v, head_dim), BF16),
            pltpu.VMEM((items, rows_t, head_dim), BF16),
        ]
        * 3
        + [
            pltpu.VMEM((3, items, rows, head_dim), BF16),
            pltpu.VMEM((3, waves, n, rows, head_dim), BF16),
            pltpu.VMEM((waves, n, rows, head_dim), BF16),
            pltpu.VMEM((items, rows, head_dim), BF16),
            pltpu.VMEM((n, rows, 2 * head_dim), BF16),
            pltpu.VMEM((2, 2, rows_v, head_dim), F32),
            pltpu.VMEM(out_weight.shape, BF16),
            pltpu.VMEM((branches, rows, width), F32),
            pltpu.SemaphoreType.DMA((4, waves, n)),
            pltpu.SemaphoreType.DMA((4, waves, n)),
            pltpu.SemaphoreType.DMA((7,)),
            pltpu.SemaphoreType.DMA((branches, width // tile)),
        ],
        compiler_params=pltpu.CompilerParams(
            collective_id=0, has_side_effects=True, vmem_limit_bytes=63 * 1024 * 1024
        ),
    )(
        flat(video_value),
        flat(text_value),
        flat(video_key),
        flat(text_key),
        flat(video_query),
        flat(text_query),
        positions,
        text_lengths,
        query_gain.reshape(1, head_dim),
        key_gain.reshape(1, head_dim),
        out_weight,
    )

    def columns(*lead):
        return pl.BlockSpec(lead + (tile,), lambda t: (0,) * len(lead) + (t,))

    return pl.pallas_call(
        finish,
        grid=(width // tile,),
        out_shape=(
            jax.ShapeDtypeStruct((rows_v, width), BF16),
            jax.ShapeDtypeStruct((branches, rows_v, width), BF16),
            jax.ShapeDtypeStruct((branches, rows_t, width), BF16),
        ),
        in_specs=[
            columns(branches, rows),
            columns(branches),
            columns(branches, rows_v),
            columns(branches, rows_t),
        ],
        out_specs=(columns(rows_v), columns(branches, rows_v), columns(branches, rows_t)),
    )(projected, branch_gates, video_stream, text_stream)


def solution(mesh):
    return jax.shard_map(
        functools.partial(body, mesh.shape["sp"]),
        mesh=mesh,
        in_specs=(
            P("grp", None, "sp", None),
            P("grp", None, "sp", None),
            P("grp", None, "sp", None),
            P("grp", None, "sp", None),
            P("grp", None, "sp", None),
            P("grp", None, "sp", None),
            P("grp", "sp"),
            P("grp"),
            P(),
            P(),
            P(),
            P("grp", None),
            P("grp", "sp", None),
            P("grp", "sp", None),
        ),
        out_specs=(P("sp", "grp"), P("grp", "sp", None), P("grp", "sp", None)),
        check_vma=False,
    )
```

```python
import functools
import math

import jax
import jax.numpy as jnp
from jax import lax
from jax.experimental import pallas as pl
from jax.experimental.pallas import tpu as pltpu
from jax.sharding import PartitionSpec as P

norm_eps = 1e-06
rope_theta = 256.0
guidance_scale = 5.0

MESH = pl.DeviceIdType.MESH
F32 = jnp.float32
BF16 = jnp.bfloat16
V, K, Q, O = 0, 1, 2, 3


def swapped(rows):
    even = lax.broadcasted_iota(jnp.int32, rows.shape, 1) % 2 == 0
    last = rows.shape[1] - 1
    return jnp.where(even, pltpu.roll(rows, last, 1), pltpu.roll(rows, 1, 1))


def rope_tables(positions, head_dim):
    frame_width = head_dim // 8
    side_width = 7 * head_dim // 16
    starts = (0, frame_width, frame_width + side_width)
    extents = (frame_width, side_width, side_width)
    tokens = positions.shape[1]
    channel = lax.broadcasted_iota(jnp.int32, (head_dim, tokens), 0)
    angles = jnp.zeros((head_dim, tokens), F32)
    for slot in range(3):
        inside = (channel >= starts[slot]) & (channel < starts[slot] + extents[slot])
        within = ((channel - starts[slot]) // 2).astype(F32)
        frequency = jnp.where(
            inside, jnp.exp(-2.0 * within / extents[slot] * math.log(rope_theta)), 0.0
        )
        angles = angles + positions[slot : slot + 1, :].astype(F32) * frequency
    return jnp.cos(angles).T, jnp.sin(angles).T


def kernel(
    n,
    heads,
    chunk,
    group,
    vv_hbm,
    tv_hbm,
    vk_hbm,
    tk_hbm,
    vq_hbm,
    tq_hbm,
    pos_ref,
    len_ref,
    qg_ref,
    kg_ref,
    weight_hbm,
    proj_hbm,
    vv_ref,
    tv_ref,
    vk_ref,
    tk_ref,
    vq_ref,
    tq_ref,
    comb,
    got,
    osend,
    ohome,
    vext,
    tables,
    weight,
    acc,
    send_sem,
    recv_sem,
    local_sem,
    out_sem,
):
    me = lax.axis_index("sp")
    items, rows_v, head_dim = vq_ref.shape
    rows_t = tq_ref.shape[1]
    rows = comb.shape[2]
    waves = items // n
    width = weight.shape[1]

    barrier = pltpu.get_barrier_semaphore()

    @pl.loop(1, n)
    def _(i):
        pl.semaphore_signal(
            barrier, inc=1, device_id={"sp": lax.rem(me + i, n)}, device_id_type=MESH
        )

    sources = (vv_hbm, tv_hbm, vk_hbm, tk_hbm, vq_hbm, tq_hbm, weight_hbm)
    places = (vv_ref, tv_ref, vk_ref, tk_ref, vq_ref, tq_ref, weight)
    loads = [
        pltpu.make_async_copy(there, here, local_sem.at[i])
        for i, (there, here) in enumerate(zip(sources, places))
    ]
    for load in loads[:6]:
        load.start()

    def copy_in(kind, wave, owner, target):
        return pltpu.make_async_remote_copy(
            src_ref=comb.at[kind, wave * n + target],
            dst_ref=got.at[kind, wave, owner],
            send_sem=send_sem.at[kind, wave, target],
            recv_sem=recv_sem.at[kind, wave, owner],
            device_id={"sp": target},
            device_id_type=MESH,
        )

    def copy_back(wave, owner, target):
        return pltpu.make_async_remote_copy(
            src_ref=osend.at[wave, target],
            dst_ref=ohome.at[wave * n + owner],
            send_sem=send_sem.at[O, wave, target],
            recv_sem=recv_sem.at[O, wave, owner],
            device_id={"sp": target},
            device_id_type=MESH,
        )

    def deal(kind, wave, make):
        @pl.loop(0, n)
        def _(i):
            target = lax.rem(me + i, n)
            video, text = make(wave * n + target)

            def put(ref):
                ref[pl.ds(0, rows_v), :] = video
                ref[pl.ds(rows_v, rows_t), :] = text
                if rows > rows_v + rows_t:
                    spare = rows - rows_v - rows_t
                    ref[pl.ds(rows_v + rows_t, spare), :] = jnp.zeros((spare, head_dim), BF16)

            @pl.when(target == me)
            def _():
                put(got.at[kind, wave, me])

            @pl.when(target != me)
            def _():
                put(comb.at[kind, wave * n + target])
                copy_in(kind, wave, me, target).start()

    def make_value(item):
        return vv_ref[item], tv_ref[item]

    def inverse_rms(wide):
        return lax.rsqrt(jnp.mean(wide * wide, axis=-1, keepdims=True) + norm_eps)

    source = lax.broadcasted_iota(jnp.int32, (head_dim, head_dim), 0)
    dest = lax.broadcasted_iota(jnp.int32, (head_dim, head_dim), 1)
    partner_of = jnp.where(
        (dest % 2 == 0) & (source == dest + 1),
        -1.0,
        jnp.where((dest % 2 == 1) & (source == dest - 1), 1.0, 0.0),
    ).astype(BF16)

    def make_normed(video_ref, text_ref, slot, gain):
        def make(item):
            raw = video_ref[item]
            wide = raw.astype(F32)
            partner = jnp.dot(raw, partner_of, preferred_element_type=F32)
            video = inverse_rms(wide) * (
                wide * tables[slot, 0] + partner * tables[slot, 1]
            )
            plain = text_ref[item].astype(F32)
            text = plain * inverse_rms(plain) * gain
            return video.astype(BF16), text.astype(BF16)

        return make

    loads[0].wait()
    loads[1].wait()
    pl.semaphore_wait(barrier, n - 1)
    deal(V, 0, make_value)

    query_gain = qg_ref[...]
    key_gain = kg_ref[...]
    cosine, sine = rope_tables(pos_ref[...], head_dim)
    for slot, gain in ((0, key_gain), (1, query_gain)):
        tall = jnp.broadcast_to(gain, (8, head_dim))
        tables[slot, 0] = cosine * gain
        tables[slot, 1] = sine * swapped(tall)[0:1, :]

    make_key = make_normed(vk_ref, tk_ref, 0, key_gain)
    make_query = make_normed(vq_ref, tq_ref, 1, query_gain)
    for load in loads[2:6]:
        load.wait()
    loads[6].start()
    for wave in range(waves):
        if wave > 0:
            deal(V, wave, make_value)
        deal(K, wave, make_key)
        deal(Q, wave, make_query)

    acc[...] = jnp.zeros_like(acc)

    score_scale = head_dim ** (-0.5) * math.log2(math.e)
    row = lax.broadcasted_iota(jnp.int32, (rows, 1), 0)
    for wave in range(waves):
        limit = len_ref[(wave * n + me) // heads]

        @pl.loop(0, n)
        def _(owner):
            @pl.when(owner != me)
            def _():
                copy_in(V, wave, owner, me).wait_recv()
                copy_in(K, wave, owner, me).wait_recv()

            text_index = owner * rows_t + row - rows_v
            live = (row < rows_v) | ((row < rows_v + rows_t) & (text_index < limit))
            counted = jnp.broadcast_to(jnp.where(live, 1.0, 0.0), (rows, head_dim)).astype(BF16)
            vext[owner, :, pl.ds(0, head_dim)] = got[V, wave, owner] * counted
            vext[owner, :, pl.ds(head_dim, head_dim)] = counted

        @pl.loop(0, n // chunk)
        def _(step):
            first = lax.rem(me // chunk + step, n // chunk) * chunk
            for j in range(chunk):

                @pl.when(first + j != me)
                def _():
                    copy_in(Q, wave, first + j, me).wait_recv()

            queries = got[Q, wave, pl.ds(first, chunk)].reshape(chunk * rows, head_dim)
            keys = got[K, wave].reshape(n * rows, head_dim)
            scores = lax.dot_general(
                queries, keys, (((1,), (1,)), ((), ())), preferred_element_type=F32
            )
            weights = jnp.exp2(scores * score_scale).astype(BF16)
            summed = jnp.dot(
                weights, vext[...].reshape(n * rows, 2 * head_dim), preferred_element_type=F32
            )
            attended = (summed[:, :head_dim] / summed[:, head_dim:]).astype(BF16)
            for j in range(chunk):
                part = attended[j * rows : (j + 1) * rows]

                @pl.when(first + j == me)
                def _():
                    ohome[wave * n + me] = part

                @pl.when(first + j != me)
                def _():
                    osend[wave, first + j] = part
                    copy_back(wave, me, first + j).start()

    loads[6].wait()
    tile = math.gcd(width, 768)
    count = heads // group

    def write(branch, t):
        columns = pl.ds(pl.multiple_of(t * tile, tile), tile)
        return pltpu.make_async_copy(
            acc.at[branch, :, columns], proj_hbm.at[branch, :, columns], out_sem.at[branch, t]
        )

    for branch in range(items // heads):
        wave, start = divmod(branch * heads, n)

        @pl.loop(0, count)
        def _(step):
            if count * group == n:
                first = lax.rem(me // group + n // group - 1 - step + count, count) * group
            else:
                first = start + step * group
            for j in range(group):

                @pl.when(first + j != me)
                def _():
                    copy_back(wave, first + j, me).wait_recv()

            item = wave * n + first
            head = item - branch * heads
            rows_in = jnp.concatenate([ohome[item + j] for j in range(group)], axis=1)

            @pl.loop(0, width // tile)
            def _(t):
                columns = pl.ds(pl.multiple_of(t * tile, tile), tile)
                depth = pl.ds(pl.multiple_of(head * head_dim, head_dim), group * head_dim)
                acc[branch, :, columns] += jnp.dot(
                    rows_in, weight[depth, columns], preferred_element_type=F32
                )

                @pl.when(step == count - 1)
                def _():
                    write(branch, t).start()

    for wave in range(waves):

        @pl.loop(1, n)
        def _(i):
            target = lax.rem(me + i, n)
            for kind in (V, K, Q):
                copy_in(kind, wave, me, target).wait_send()
            copy_back(wave, me, target).wait_send()

    for branch in range(items // heads):
        for t in range(width // tile):
            write(branch, t).wait()


def finish(proj_ref, gate_ref, vstream_ref, tstream_ref, guided_ref, vnext_ref, tnext_ref):
    rows_v, rows_t = vstream_ref.shape[1], tstream_ref.shape[1]
    streams = []
    for branch in range(2):
        gate = gate_ref[branch : branch + 1, :]
        stream = vstream_ref[branch].astype(F32) + gate * proj_ref[branch, :rows_v]
        vnext_ref[branch] = stream.astype(BF16)
        streams.append(stream)
        tnext_ref[branch] = (
            tstream_ref[branch].astype(F32) + gate * proj_ref[branch, rows_v : rows_v + rows_t]
        ).astype(BF16)
    guided_ref[...] = (streams[1] + guidance_scale * (streams[0] - streams[1])).astype(BF16)


def body(
    n,
    video_query,
    video_key,
    video_value,
    text_query,
    text_key,
    text_value,
    positions,
    text_lengths,
    query_gain,
    key_gain,
    out_weight,
    branch_gates,
    video_stream,
    text_stream,
):
    branches, heads, rows_v, head_dim = video_query.shape
    rows_t = text_query.shape[2]
    items = branches * heads
    waves = items // n
    rows = -(-(rows_v + rows_t) // 16) * 16
    width = out_weight.shape[1]
    chunk = 2 if n % 2 == 0 else 1
    group = math.gcd(math.gcd(n, heads), 4)

    def flat(tensor):
        return tensor.reshape((items,) + tensor.shape[2:])

    vmem = pl.BlockSpec(memory_space=pltpu.VMEM)
    smem = pl.BlockSpec(memory_space=pltpu.SMEM)
    anywhere = pl.BlockSpec(memory_space=pl.ANY)
    tile = math.gcd(width, 768)
    projected = pl.pallas_call(
        functools.partial(kernel, n, heads, chunk, group),
        out_shape=jax.ShapeDtypeStruct((branches, rows, width), F32),
        in_specs=[anywhere] * 6 + [vmem, smem, vmem, vmem, anywhere],
        out_specs=anywhere,
        scratch_shapes=[
            pltpu.VMEM((items, rows_v, head_dim), BF16),
            pltpu.VMEM((items, rows_t, head_dim), BF16),
        ]
        * 3
        + [
            pltpu.VMEM((3, items, rows, head_dim), BF16),
            pltpu.VMEM((3, waves, n, rows, head_dim), BF16),
            pltpu.VMEM((waves, n, rows, head_dim), BF16),
            pltpu.VMEM((items, rows, head_dim), BF16),
            pltpu.VMEM((n, rows, 2 * head_dim), BF16),
            pltpu.VMEM((2, 2, rows_v, head_dim), F32),
            pltpu.VMEM(out_weight.shape, BF16),
            pltpu.VMEM((branches, rows, width), F32),
            pltpu.SemaphoreType.DMA((4, waves, n)),
            pltpu.SemaphoreType.DMA((4, waves, n)),
            pltpu.SemaphoreType.DMA((7,)),
            pltpu.SemaphoreType.DMA((branches, width // tile)),
        ],
        compiler_params=pltpu.CompilerParams(
            collective_id=0, has_side_effects=True, vmem_limit_bytes=63 * 1024 * 1024
        ),
    )(
        flat(video_value),
        flat(text_value),
        flat(video_key),
        flat(text_key),
        flat(video_query),
        flat(text_query),
        positions,
        text_lengths,
        query_gain.reshape(1, head_dim),
        key_gain.reshape(1, head_dim),
        out_weight,
    )

    step = math.gcd(width, 512)

    def columns(*lead):
        return pl.BlockSpec(lead + (step,), lambda t: (0,) * len(lead) + (t,))

    return pl.pallas_call(
        finish,
        grid=(width // step,),
        out_shape=(
            jax.ShapeDtypeStruct((rows_v, width), BF16),
            jax.ShapeDtypeStruct((branches, rows_v, width), BF16),
            jax.ShapeDtypeStruct((branches, rows_t, width), BF16),
        ),
        in_specs=[
            columns(branches, rows),
            columns(branches),
            columns(branches, rows_v),
            columns(branches, rows_t),
        ],
        out_specs=(columns(rows_v), columns(branches, rows_v), columns(branches, rows_t)),
    )(projected, branch_gates, video_stream, text_stream)


def solution(mesh):
    return jax.shard_map(
        functools.partial(body, mesh.shape["sp"]),
        mesh=mesh,
        in_specs=(
            P("grp", None, "sp", None),
            P("grp", None, "sp", None),
            P("grp", None, "sp", None),
            P("grp", None, "sp", None),
            P("grp", None, "sp", None),
            P("grp", None, "sp", None),
            P("grp", "sp"),
            P("grp"),
            P(),
            P(),
            P(),
            P("grp", None),
            P("grp", "sp", None),
            P("grp", "sp", None),
        ),
        out_specs=(P("sp", "grp"), P("grp", "sp", None), P("grp", "sp", None)),
        check_vma=False,
    )
```
